1024 devices in a mesh: gx: 16 (over x, core), gy: 8 (over y), gz: 8 (over z).
Axes of the slice: x: 8, y: 8, z: 8, core: 2. Of those that a mesh axis runs over, the one named last changes fastest.
Arguments:
- coarse_pdfs: float32 [19, 64, 32, 512], P(None, 'gx', 'gy', 'gz'), may hold values from 0.1 to 32
- fine_pdfs: float32 [19, 64, 64, 1024], P(None, 'gx', 'gy', 'gz'), may hold values from 0.1 to 32
- centers: int32 [3, 3, 4, 4, 16], replicated, may hold values from 4 to 59, as said below
- sphere_velocity: float32 [3, 4, 4, 16], replicated, may hold values from -0.05 to 0.05
Outputs:
- coarse_next: float32 [19, 64, 32, 512], P(None, 'gx', 'gy', 'gz')
- fine_next: float32 [19, 64, 64, 1024], P(None, 'gx', 'gy', 'gz')
- sphere_force: float32 [2, 3, 4, 4, 16], replicated
The draws below stay inside these ranges and needn't reach their ends.
Inputs may be any that keep to these rules, and one draw needn't show every extreme that they name: `centers`: each coordinate of a center is counted from its box's first cell; from one substep to the next it changes by -1, 0 or 1, and the same change repeats in the second substep.
All inputs are finite; a program needn't handle non-finite values.
Results may differ from the reference program's by a relative error of at most 0.0003.
Values sent between devices are 32-bit elements; how exact they have to be, the bound alone decides.
No kernel may reach another device: no remote copies, remote signals or barrier semaphores. Data moves between devices by JAX's collectives and lax.ppermute only.
A program may use at most 32 MiB of HBM per device.

```python
import jax
import jax.numpy as jnp
from jax import lax

BOX_XY = 16
BOX_Z = 64
RADIUS = 4
NX = 64
NY = 32
NZ = 512
FINE_X = 64
FINE_Y = 64
FINE_Z = 1024
NBX = 4
NBY = 4
NBZ = 16


VELOCITIES = ((0, 0, 0), (1, 0, 0), (-1, 0, 0), (0, 1, 0), (0, -1, 0), (0, 0, 1), (0, 0, -1), (1, 1, 0), (-1, -1, 0), (1, -1, 0), (-1, 1, 0), (1, 0, 1), (-1, 0, -1), (1, 0, -1), (-1, 0, 1), (0, 1, 1), (0, -1, -1), (0, 1, -1), (0, -1, 1))


WEIGHTS = (1.0 / 3.0,) + (1.0 / 18.0,) * 6 + (1.0 / 36.0,) * 12


def population_field(key, extent_x, extent_y, extent_z):
    subkeys = jax.random.split(key, 3)
    density = jax.random.uniform(subkeys[0], (extent_x, extent_y, extent_z), jnp.float32, 20.0, 52.0)
    velocity = jax.random.uniform(subkeys[1], (3, extent_x, extent_y, extent_z), jnp.float32, -0.06, 0.06)
    jitter = jax.random.uniform(subkeys[2], (19, extent_x, extent_y, extent_z), jnp.float32, -0.3, 0.3)
    speed_sq = velocity[0] * velocity[0] + velocity[1] * velocity[1] + velocity[2] * velocity[2]
    populations = []
    for direction in range(19):
        projected = VELOCITIES[direction][0] * velocity[0] + VELOCITIES[direction][1] * velocity[1] + VELOCITIES[direction][2] * velocity[2]
        populations.append(WEIGHTS[direction] * density * (1.0 + 3.0 * projected + 4.5 * projected * projected - 1.5 * speed_sq + jitter[direction]))
    return jnp.stack(populations)


def draw_coarse_pdfs(key, part):
    return population_field(jax.random.fold_in(key, 101), NX, NY, NZ)


def draw_fine_pdfs(key, part):
    return population_field(jax.random.fold_in(key, 202), FINE_X, FINE_Y, FINE_Z)


def draw_centers(key, part):
    subkeys = jax.random.split(jax.random.fold_in(key, 303), 2)
    limits = jnp.array([BOX_XY, BOX_XY, BOX_Z], dtype=jnp.int32)[:, None, None, None]
    starts = jax.random.randint(subkeys[0], (3, NBX, NBY, NBZ), RADIUS + 2, limits - RADIUS - 2, dtype=jnp.int32)
    motion = jax.random.randint(subkeys[1], (3, NBX, NBY, NBZ), -1, 2, dtype=jnp.int32)
    return jnp.stack([starts, starts + motion, starts + 2 * motion])


def setup_inputs(seed: int = 0) -> dict:
    splits = jax.random.split(jax.random.key(seed), 5)
    coarse_pdfs = draw_coarse_pdfs(jax.random.fold_in(splits[4], 71), 0)
    fine_pdfs = draw_fine_pdfs(jax.random.fold_in(splits[4], 71), 0)
    centers = draw_centers(jax.random.fold_in(splits[4], 71), 0)
    sphere_velocity = jnp.clip(jax.random.uniform(splits[3], (3, NBX, NBY, NBZ), jnp.float32, -0.05, 0.05), -0.05, 0.05)
    return {"coarse_pdfs": coarse_pdfs, "fine_pdfs": fine_pdfs, "centers": centers, "sphere_velocity": sphere_velocity}


VELOCITIES = ((0, 0, 0), (1, 0, 0), (-1, 0, 0), (0, 1, 0), (0, -1, 0), (0, 0, 1), (0, 0, -1), (1, 1, 0), (-1, -1, 0), (1, -1, 0), (-1, 1, 0), (1, 0, 1), (-1, 0, -1), (1, 0, -1), (-1, 0, 1), (0, 1, 1), (0, -1, -1), (0, 1, -1), (0, -1, 1))
OPPOSITE = (0, 2, 1, 4, 3, 6, 5, 8, 7, 10, 9, 12, 11, 14, 13, 16, 15, 18, 17)
WEIGHTS = (1.0 / 3.0,) + (1.0 / 18.0,) * 6 + (1.0 / 36.0,) * 12
COARSE_RATE = 1.25
FINE_RATE = 1.0 / 1.1
HIGHEST = lax.Precision.HIGHEST


def project(vectors, direction):
    projected = jnp.zeros_like(vectors[0])
    for dimension in range(3):
        sign = VELOCITIES[direction][dimension]
        if sign == 1:
            projected = projected + vectors[dimension]
        elif sign == -1:
            projected = projected - vectors[dimension]
    return projected


def speed_squared(vectors):
    return vectors[0] * vectors[0] + vectors[1] * vectors[1] + vectors[2] * vectors[2]


def equilibrium(density, vectors, speed_sq, direction):
    projected = project(vectors, direction)
    return WEIGHTS[direction] * density * (1.0 + 3.0 * projected + 4.5 * projected * projected - 1.5 * speed_sq)


def total_density(populations):
    density = populations[0]
    for direction in range(1, 19):
        density = density + populations[direction]
    return density


def collide(populations, relaxation):
    density = total_density(populations)
    velocity = []
    for dimension in range(3):
        summed = jnp.zeros_like(density)
        for direction in range(19):
            sign = VELOCITIES[direction][dimension]
            if sign == 1:
                summed = summed + populations[direction]
            elif sign == -1:
                summed = summed - populations[direction]
        velocity.append(summed / density)
    speed_sq = speed_squared(velocity)
    relaxed = []
    for direction in range(19):
        target = equilibrium(density, velocity, speed_sq, direction)
        relaxed.append(populations[direction] - relaxation * (populations[direction] - target))
    return jnp.stack(relaxed)


def box_onehot(coords, box_size, box_count):
    box_index = jnp.floor_divide(coords, box_size)
    onehot = (box_index[None, :] == jnp.arange(box_count, dtype=jnp.int32)[:, None]).astype(jnp.float32)
    offsets = (coords - box_index * box_size).astype(jnp.float32)
    return onehot, offsets


def geometry(coord_x, coord_y, coord_z, centers, sphere_velocity):
    count_x, count_y, count_z = centers.shape[2], centers.shape[3], centers.shape[4]
    table_x, offset_x = box_onehot(coord_x, BOX_XY, count_x)
    table_y, offset_y = box_onehot(coord_y, BOX_XY, count_y)
    table_z, offset_z = box_onehot(coord_z, BOX_Z, count_z)
    inside = ((coord_x >= 0) & (coord_x < count_x * BOX_XY))[:, None, None]

    def spread(values):
        return jnp.einsum("abc,ax,by,cz->xyz", values, table_x, table_y, table_z, precision=HIGHEST)

    solids = []
    for moment in range(3):
        gap_x = offset_x[:, None, None] - spread(centers[moment, 0].astype(jnp.float32))
        gap_y = offset_y[None, :, None] - spread(centers[moment, 1].astype(jnp.float32))
        gap_z = offset_z[None, None, :] - spread(centers[moment, 2].astype(jnp.float32))
        distance = gap_x * gap_x + gap_y * gap_y + gap_z * gap_z
        solids.append((distance <= float(RADIUS * RADIUS)) & inside)
    velocity_field = [spread(sphere_velocity[dimension]) for dimension in range(3)]
    return solids, velocity_field


def pull_from(values, direction):
    step_x, step_y, step_z = VELOCITIES[direction]
    width_x = values.shape[-3] - 2
    sliced = values[..., 1 - step_x:1 - step_x + width_x, :, :]
    return jnp.roll(sliced, (step_y, step_z), axis=(-2, -1))


def upsample(ghost_plane):
    return jnp.repeat(jnp.repeat(ghost_plane, 2, axis=1), 2, axis=2)


def coalesce(ghost_plane):
    grouped = ghost_plane.reshape(19, ghost_plane.shape[1] // 2, 2, ghost_plane.shape[2] // 2, 2)
    return (grouped[:, :, 0, :, 0] + grouped[:, :, 1, :, 0] + grouped[:, :, 0, :, 1] + grouped[:, :, 1, :, 1]) * 0.25


def substep(padded, solid_prev, solid_new, velocity_field):
    interior = padded[:, 1:-1]
    density = total_density(padded)
    density_in = density[1:-1]
    open_cells = jnp.logical_not(solid_prev) & jnp.logical_not(solid_new)
    moving = open_cells[1:-1]
    numerator = WEIGHTS[0] * density_in
    denominator = jnp.full(density_in.shape, WEIGHTS[0], jnp.float32)
    arrived = [interior[0]]
    push_sums = [jnp.zeros(density_in.shape, jnp.float32) for dimension in range(3)]
    for direction in range(1, 19):
        step_x, step_y, step_z = VELOCITIES[direction]
        solid_next = pull_from(solid_new, direction)
        neighbour_velocity = [pull_from(values, direction) for values in velocity_field]
        returned = interior[OPPOSITE[direction]]
        bounced = returned + 6.0 * WEIGHTS[direction] * density_in * project(neighbour_velocity, direction)
        arrived.append(jnp.where(solid_next, bounced, pull_from(padded[direction], direction)))
        link_term = jnp.where(solid_next & moving, returned + bounced, 0.0)
        pushed = jnp.roll(link_term, (-step_x, -step_y, -step_z), axis=(0, 1, 2))
        for dimension in range(3):
            sign = VELOCITIES[direction][dimension]
            if sign == 1:
                push_sums[dimension] = push_sums[dimension] - pushed
            elif sign == -1:
                push_sums[dimension] = push_sums[dimension] + pushed
        open_next = pull_from(open_cells, direction).astype(jnp.float32)
        numerator = numerator + WEIGHTS[direction] * pull_from(density, direction) * open_next
        denominator = denominator + WEIGHTS[direction] * open_next
    refill_density = numerator / denominator
    own_velocity = [values[1:-1] for values in velocity_field]
    speed_sq = speed_squared(own_velocity)
    covered = solid_new[1:-1]
    uncovered = solid_prev[1:-1]
    updated = []
    for direction in range(19):
        refill = equilibrium(refill_density, own_velocity, speed_sq, direction)
        updated.append(jnp.where(covered, interior[direction], jnp.where(uncovered, refill, arrived[direction])))
    stacked = jnp.stack(push_sums).reshape(3, NBX, BOX_XY, NBY, BOX_XY, NBZ, BOX_Z)
    forces = jnp.sum(stacked, axis=(2, 4, 6))
    return jnp.stack(updated), forces


def reference(coarse_pdfs, fine_pdfs, centers, sphere_velocity):
    coord_x = jnp.arange(-1, FINE_X + 1, dtype=jnp.int32)
    coord_y = jnp.arange(FINE_Y, dtype=jnp.int32)
    coord_z = jnp.arange(FINE_Z, dtype=jnp.int32)
    solids, velocity_field = geometry(coord_x, coord_y, coord_z, centers, sphere_velocity)
    coarse_post = collide(coarse_pdfs, COARSE_RATE)
    left_fill = upsample(coarse_post[:, NX - 1])
    right_fill = upsample(coarse_post[:, 0])
    first_post = collide(fine_pdfs, FINE_RATE)
    left_coal = coalesce(first_post[:, FINE_X - 1])
    right_coal = coalesce(first_post[:, 0])

    def extended(fresh):
        return jnp.concatenate([left_fill[:, None], fresh, right_fill[:, None]], axis=1)

    middle, first_forces = substep(extended(first_post), solids[0], solids[1], velocity_field)
    fine_next, second_forces = substep(extended(collide(middle, FINE_RATE)), solids[1], solids[2], velocity_field)
    coarse_ready = jnp.concatenate([left_coal[:, None], coarse_post, right_coal[:, None]], axis=1)
    coarse_next = jnp.stack([pull_from(coarse_ready[direction], direction) for direction in range(19)])
    return coarse_next, fine_next, jnp.stack([first_forces, second_forces])
```

```python
import jax
import jax.numpy as jnp
from jax import lax
from jax.experimental import pallas as pl
from jax.experimental.pallas import tpu as pltpu
from jax.sharding import Mesh
from jax.sharding import PartitionSpec as P

BOX_XY = 16
BOX_Z = 64
RADIUS = 4
GX = ("gx_0", "gx_1")

VELOCITIES = (
    (0, 0, 0),
    (1, 0, 0),
    (-1, 0, 0),
    (0, 1, 0),
    (0, -1, 0),
    (0, 0, 1),
    (0, 0, -1),
    (1, 1, 0),
    (-1, -1, 0),
    (1, -1, 0),
    (-1, 1, 0),
    (1, 0, 1),
    (-1, 0, -1),
    (1, 0, -1),
    (-1, 0, 1),
    (0, 1, 1),
    (0, -1, -1),
    (0, 1, -1),
    (0, -1, 1),
)
OPPOSITE = (0, 2, 1, 4, 3, 6, 5, 8, 7, 10, 9, 12, 11, 14, 13, 16, 15, 18, 17)
WEIGHTS = (1.0 / 3.0,) + (1.0 / 18.0,) * 6 + (1.0 / 36.0,) * 12
COARSE_RATE = 1.25
FINE_RATE = 1.0 / 1.1
HIGHEST = lax.Precision.HIGHEST
RHO = 19
BIG = 1.0e30


def heading(axis, sign):
    return tuple(q for q in range(19) if VELOCITIES[q][axis] == sign)


XP, XM = heading(0, 1), heading(0, -1)
YP, YM = heading(1, 1), heading(1, -1)
ZP, ZM = heading(2, 1), heading(2, -1)
F32 = jnp.float32
VMEM = pl.BlockSpec(memory_space=pltpu.VMEM)
SMEM = pl.BlockSpec(memory_space=pltpu.SMEM)


def along(vectors, q):
    total = None
    for d in range(3):
        sign = VELOCITIES[q][d]
        if sign == 0:
            continue
        if total is None:
            total = vectors[d] if sign == 1 else -vectors[d]
        else:
            total = total + vectors[d] if sign == 1 else total - vectors[d]
    return total


def equilibria(density, vectors):
    base = 1.0 - 1.5 * (
        vectors[0] * vectors[0] + vectors[1] * vectors[1] + vectors[2] * vectors[2]
    )
    scaled = {w: w * density for w in set(WEIGHTS)}
    out = [scaled[WEIGHTS[0]] * base]
    for q in range(1, 19, 2):
        c = along(vectors, q)
        even = base + 4.5 * c * c
        odd = 3.0 * c
        out.append(scaled[WEIGHTS[q]] * (even + odd))
        out.append(scaled[WEIGHTS[q]] * (even - odd))
    return out


def collided(p, rate):
    density = p[0]
    for q in range(1, 19):
        density = density + p[q]
    inverse = 1.0 / density
    vectors = []
    for d in range(3):
        total = None
        for q in range(19):
            sign = VELOCITIES[q][d]
            if sign == 1:
                total = p[q] if total is None else total + p[q]
        for q in range(19):
            if VELOCITIES[q][d] == -1:
                total = total - p[q]
        vectors.append(total * inverse)
    targets = equilibria(density, vectors)
    return [p[q] - rate * (p[q] - targets[q]) for q in range(19)], density


def dot(a, b):
    return lax.dot_general(
        a, b, (((1,), (0,)), ((), ())), precision=HIGHEST, preferred_element_type=F32
    )


def iota2(shape, axis):
    return lax.broadcasted_iota(jnp.int32, shape, axis)


def upsampled(tiles):
    rows = tiles.shape[0]
    r, c = iota2((rows, rows), 0), iota2((rows, rows), 1)
    left = jnp.where(((r >> 3) == (c >> 3)) & (((r & 7) >> 1) == (c & 7)), 1.0, 0.0)
    k, n = iota2((128, 128), 0), iota2((128, 128), 1)
    right = jnp.where(k == (n >> 1), 1.0, 0.0)
    return dot(left, dot(tiles, right))


def coalesced(tiles):
    rows = tiles.shape[0]
    r, c = iota2((rows, rows), 0), iota2((rows, rows), 1)
    left = jnp.where(((r >> 3) == (c >> 3)) & ((r & 7) == ((c & 7) >> 1)), 0.25, 0.0)
    k, n = iota2((128, 128), 0), iota2((128, 128), 1)
    right = jnp.where((k >> 1) == n, 1.0, 0.0)
    return dot(left, dot(tiles, right))


def collide_kernel(fine, coarse, fp, cp, xr, xl):
    gx = lax.axis_index(GX)
    last = lax.axis_size(GX) - 1
    cp[...] = jnp.zeros(cp.shape, F32)
    for x in range(4):
        post, density = collided([coarse[q, x] for q in range(19)], COARSE_RATE)
        for q in range(19):
            cp[q, x, 0:4, 0:64] = post[q]

    def plane(x, carry):
        post, density = collided([fine[q, x] for q in range(19)], FINE_RATE)
        for q in range(19):
            fp[q, x] = post[q]
        fp[RHO, x] = density
        return carry

    lax.fori_loop(0, 4, plane, 0)
    for out, near, far, inward, edge in ((xr, 3, 2, XP, last), (xl, 0, 1, XM, 0)):
        for k, q in enumerate(inward):
            out[19 + k] = fp[q, far]
        out[24] = fp[RHO, far]

        @pl.when(gx != edge)
        def _():
            out[0:19] = fp[0:19, near]
            for k, q in enumerate(inward):
                out[25 + k] = cp[q, near]

        @pl.when(gx == edge)
        def _():
            up = upsampled(cp[:, near].reshape(152, 128))
            out[0:19] = up.reshape(19, 8, 128)
            picked = jnp.concatenate([fp[q, near] for q in inward], axis=0)
            out[25:30] = coalesced(picked).reshape(5, 8, 128)


def pack_y_kernel(fp, cp, r_l, r_r, yr, yl):
    rho_l, rho_r = r_l[0], r_r[0]
    for q in range(1, 19):
        rho_l = rho_l + r_l[q]
        rho_r = rho_r + r_r[q]
    for out, near, far, cnear, inward in ((yr, 7, 6, 3, YP), (yl, 0, 1, 0, YM)):
        out[...] = jnp.zeros(out.shape, F32)
        out[0:19, 1:2] = r_l[0:19, near : near + 1]
        out[RHO, 1:2] = rho_l[near : near + 1]
        out[0:19, 6:7] = r_r[0:19, near : near + 1]
        out[RHO, 6:7] = rho_r[near : near + 1]
        for x in range(4):
            out[0:20, 2 + x : 3 + x] = fp[:, x, near : near + 1]
        for k in range(5):
            out[XP[k], 0:1] = r_l[19 + k, near : near + 1]
            out[XM[k], 7:8] = r_r[19 + k, near : near + 1]
        out[RHO, 0:1] = r_l[24, near : near + 1]
        out[RHO, 7:8] = r_r[24, near : near + 1]
        for k, q in enumerate(inward):
            out[20 + k, 1:2] = r_l[q, far : far + 1]
            out[20 + k, 6:7] = r_r[q, far : far + 1]
            for x in range(4):
                out[20 + k, 2 + x : 3 + x] = fp[q, x, far : far + 1]
                out[26 + k, 1 + x : 2 + x] = cp[q, x, cnear : cnear + 1]
            if q in XP:
                out[20 + k, 0:1] = r_l[19 + XP.index(q), far : far + 1]
                out[26 + k, 0:1] = r_l[25 + XP.index(q), cnear : cnear + 1]
            if q in XM:
                out[20 + k, 7:8] = r_r[19 + XM.index(q), far : far + 1]
                out[26 + k, 5:6] = r_r[25 + XM.index(q), cnear : cnear + 1]
        out[25, 0:1] = r_l[24, far : far + 1]
        out[25, 1:2] = rho_l[far : far + 1]
        out[25, 6:7] = rho_r[far : far + 1]
        out[25, 7:8] = r_r[24, far : far + 1]
        for x in range(4):
            out[25, 2 + x : 3 + x] = fp[RHO, x, far : far + 1]


def pack_z_kernel(fp, cp, r_l, r_r, y_l, y_r, ext, cext, zr, zl):
    for x in range(4):
        ext[:, 2 + x, 0:8] = fp[:, x]
        cext[:, 1 + x] = cp[:, x]
    cext[:, 0] = jnp.zeros((19, 8, 128), F32)
    cext[:, 5] = jnp.zeros((19, 8, 128), F32)
    for got, near, far, cplane, inward in ((r_l, 1, 0, 0, XP), (r_r, 6, 7, 5, XM)):
        ext[0:19, near, 0:8] = got[0:19]
        density = got[0]
        for q in range(1, 19):
            density = density + got[q]
        ext[RHO, near, 0:8] = density
        for k, q in enumerate(inward):
            ext[q, far, 0:8] = got[19 + k]
            cext[q, cplane] = got[25 + k]
        ext[RHO, far, 0:8] = got[24]
    for j in range(8):
        for got, near, far, crow, inward in ((y_l, 15, 14, 7, YP), (y_r, 8, 9, 4, YM)):
            ext[:, j, near : near + 1] = got[0:20, j : j + 1]
            for k, q in enumerate(inward):
                ext[q, j, far : far + 1] = got[20 + k, j : j + 1]
                if j < 6:
                    cext[q, j, crow : crow + 1] = got[26 + k, j : j + 1]
            ext[RHO, j, far : far + 1] = got[25, j : j + 1]
    lane = iota2((8, 128), 1)

    def plane(j, carry):
        for h in range(2):
            to_r = jnp.zeros((8, 128), F32)
            to_l = jnp.zeros((8, 128), F32)
            for f in range(20):
                turned = pltpu.roll(ext[f, j, 8 * h : 8 * h + 8], (2 * f + 2) % 128, 1)
                to_r = jnp.where((lane >> 1) == f, turned, to_r)
                to_l = jnp.where((lane >> 1) == f + 1, turned, to_l)
            if h == 0:
                jc = jnp.minimum(j, 5)
                for k in range(5):
                    to_r = jnp.where(lane == 64 + k, pltpu.roll(cext[ZP[k], jc], k + 1, 1), to_r)
                    to_l = jnp.where(lane == 64 + k, pltpu.roll(cext[ZM[k], jc], 64 + k, 1), to_l)
            zr[j, 8 * h : 8 * h + 8] = to_r
            zl[j, 8 * h : 8 * h + 8] = to_l
        return carry

    lax.fori_loop(0, 8, plane, 0)


def geometry_kernel(centers, velocity, code, wind):
    gx, gy, gz = lax.axis_index(GX), lax.axis_index("gy"), lax.axis_index("gz")
    row, lane = iota2((8, 128), 0), iota2((8, 128), 1)
    low_row, low_lane = row < 4, lane < 64
    nbx, nby, nbz = 4, 4, 16
    boxes = nbx * nby * nbz
    y0, z0, x0 = gy * 8, gz * 128, gx * 4
    own_y = y0 // BOX_XY
    prev_y = lax.rem(lax.div(y0 + nby * BOX_XY - 1, BOX_XY), nby)
    next_y = lax.rem(lax.div(y0 + 8, BOX_XY), nby)
    lo_z = z0 // BOX_Z
    prev_z = lax.rem(lo_z + nbz - 1, nbz)
    next_z = lax.rem(lo_z + 2, nbz)
    row_boxes = ((own_y, own_y), (next_y, prev_y))
    lane_boxes = ((lo_z, lo_z + 1), (next_z, prev_z))
    y_of = (row, jnp.where(low_row, row + 8, row - 8))
    z_of = (lane, jnp.where(low_lane, lane + 128, lane - 128))
    off_y = [((y0 + y_of[h] + BOX_XY * nby) & (BOX_XY - 1)).astype(F32) for h in range(2)]
    off_z = [((z0 + z_of[h] + BOX_Z * nbz) & (BOX_Z - 1)).astype(F32) for h in range(2)]

    def plane(j, carry):
        x = x0 + j - 2
        inside = jnp.where((x >= 0) & (x < nbx * BOX_XY), 1.0, 0.0)
        safe = jnp.clip(x, 0, nbx * BOX_XY - 1)
        bx = lax.div(safe, BOX_XY)
        off_x = lax.rem(safe, BOX_XY).astype(F32)

        def field(table, base, h, g):
            def one(by, bz):
                return table[base + (bx * nby + by) * nbz + bz].astype(F32)

            upper = jnp.where(
                low_lane,
                one(row_boxes[h][0], lane_boxes[g][0]),
                one(row_boxes[h][0], lane_boxes[g][1]),
            )
            if h == 0:
                return upper
            lower = jnp.where(
                low_lane,
                one(row_boxes[h][1], lane_boxes[g][0]),
                one(row_boxes[h][1], lane_boxes[g][1]),
            )
            return jnp.where(low_row, upper, lower)

        for h in range(2):
            for g in range(2):
                bits = jnp.zeros((8, 128), F32)
                for moment in range(3):
                    base = moment * 3 * boxes
                    gap_x = off_x - field(centers, base, h, g)
                    gap_y = off_y[h] - field(centers, base + boxes, h, g)
                    gap_z = off_z[g] - field(centers, base + 2 * boxes, h, g)
                    distance = gap_x * gap_x + gap_y * gap_y + gap_z * gap_z
                    hit = (distance <= float(RADIUS * RADIUS)) & (inside > 0.5)
                    bits = bits + jnp.where(hit, float(1 << moment), 0.0)
                code[j, h, g] = bits
                for d in range(3):
                    wind[d, j, h, g] = field(velocity, d * boxes, h, g) * inside
        return carry

    lax.fori_loop(0, 8, plane, 0)


def turned(tiles, step, axis):
    size = 8 if axis == 0 else 128
    at = iota2((8, 128), axis)
    rolled = [pltpu.roll(t, step % size, axis) for t in tiles]
    seam = at == (0 if step == 1 else size - 1)
    return [jnp.where(seam, rolled[1], rolled[0]), jnp.where(seam, rolled[0], rolled[1])]


def pull(tiles, cy, cz):
    if cz:
        tiles = [turned(tiles[h], cz, 1) for h in range(2)]
    if cy:
        first = turned([tiles[0][0], tiles[1][0]], cy, 0)
        second = turned([tiles[0][1], tiles[1][1]], cy, 0)
        tiles = [[first[0], second[0]], [first[1], second[1]]]
    return tiles


def main_kernel(ext_a, cext, z_l, z_r, code, wind, fine_next, coarse_next, force, ext_b, post, sums):
    gx, gz = lax.axis_index(GX), lax.axis_index("gz")
    last = lax.axis_size(GX) - 1
    row, lane = iota2((8, 128), 0), iota2((8, 128), 1)

    for k in range(5):
        q = ZP[k]
        for x in range(4):
            j = 1 + x - VELOCITIES[q][0]
            tile = jnp.where(lane == 127, pltpu.roll(z_l[j, 0:8], 63 - k, 1), cext[q, j])
            tile = pltpu.roll(tile, 1, 1)
            if VELOCITIES[q][1]:
                tile = pltpu.roll(tile, VELOCITIES[q][1] % 8, 0)
            coarse_next[q, x] = tile[0:4, 0:64]
        q = ZM[k]
        for x in range(4):
            j = 1 + x - VELOCITIES[q][0]
            tile = z_r[j, 0:8]
            if k:
                tile = pltpu.roll(tile, 128 - k, 1)
            tile = jnp.where(lane == 64, tile, cext[q, j])
            tile = pltpu.roll(tile, 127, 1)
            if VELOCITIES[q][1]:
                tile = pltpu.roll(tile, VELOCITIES[q][1] % 8, 0)
            coarse_next[q, x] = tile[0:4, 0:64]
    for q in range(19):
        if VELOCITIES[q][2] == 0:
            for x in range(4):
                tile = cext[q, 1 + x - VELOCITIES[q][0]]
                if VELOCITIES[q][1]:
                    tile = pltpu.roll(tile, VELOCITIES[q][1] % 8, 0)
                coarse_next[q, x] = tile[0:4, 0:64]

    def unpack(j, carry):
        for h in range(2):
            from_l = z_l[j, 8 * h : 8 * h + 8]
            from_r = z_r[j, 8 * h : 8 * h + 8]
            for f in range(20):
                before = pltpu.roll(from_l, (126 - 2 * f) % 128, 1)
                after = pltpu.roll(from_r, (126 - 2 * f) % 128, 1)
                ext_b[f, j, 8 * h : 8 * h + 8] = jnp.where(lane < 64, after, before)
        return carry

    lax.fori_loop(0, 8, unpack, 0)

    def substep(get, prev_bit, new_bit, first, stop, store, halves):
        def bits(j, h, g):
            return code[j, h, g].astype(jnp.int32)

        def prepare(j, carry):
            rho_open, open_ = [[None] * 2, [None] * 2], [[None] * 2, [None] * 2]
            for h in range(2):
                for g in range(2):
                    is_open = (bits(j, h, g) & (prev_bit | new_bit)) == 0
                    open_[h][g] = jnp.where(is_open, 1.0, 0.0)
                    rho_open[h][g] = jnp.where(is_open, get(RHO, j, h, g), 0.0)
            for n, tiles in enumerate((rho_open, open_)):
                back, forth = pull(tiles, 0, 1), pull(tiles, 0, -1)
                side_z = [[back[h][g] + forth[h][g] for g in range(2)] for h in range(2)]
                down, up = pull(tiles, 1, 0), pull(tiles, -1, 0)
                down2, up2 = pull(side_z, 1, 0), pull(side_z, -1, 0)
                for h in halves:
                    for g in halves:
                        side_y = down[h][g] + up[h][g]
                        both = down2[h][g] + up2[h][g]
                        sums[2 * n, j, h, g] = 2.0 * (side_y + side_z[h][g]) + both
                        sums[2 * n + 1, j, h, g] = 2.0 * tiles[h][g] + side_y + side_z[h][g]
            return carry

        lax.fori_loop(first - 1, stop + 1, prepare, 0)

        def plane(j, carry):
            pushes = list(carry)
            mine = [[bits(j, h, g) for g in range(2)] for h in range(2)]
            rho = [[get(RHO, j, h, g) for g in range(2)] for h in range(2)]
            covered, uncovered, refill = {}, {}, {}
            for h in halves:
                for g in halves:
                    covered[h, g] = (mine[h][g] & new_bit) != 0
                    uncovered[h, g] = (mine[h][g] & prev_bit) != 0
                    above = (
                        12.0 * rho[h][g]
                        + sums[0, j, h, g]
                        + (sums[1, j - 1, h, g] + sums[1, j + 1, h, g])
                    )
                    below = 12.0 + sums[2, j, h, g] + (sums[3, j - 1, h, g] + sums[3, j + 1, h, g])
                    density = above / below
                    own = [wind[d, j, h, g] for d in range(3)]
                    refill[h, g] = equilibria(density, own)
            own = [wind[d, j, 0, 0] for d in range(3)]
            for q in range(19):
                cx, cy, cz = VELOCITIES[q]
                weight = 6.0 * WEIGHTS[q]
                if q == 0:
                    for h in halves:
                        for g in halves:
                            p0 = get(0, j, h, g)
                            kept = jnp.where(uncovered[h, g], refill[h, g][0], p0)
                            store(0, j, h, g, jnp.where(covered[h, g], p0, kept))
                    continue
                src = j - cx
                ghost = jnp.logical_or(
                    jnp.logical_and(gx == 0, src < 2), jnp.logical_and(gx == last, src > 5)
                )
                fluid = jnp.where(ghost, 2.0 * BIG, BIG)
                state = [[None] * 2, [None] * 2]
                for h in range(2):
                    for g in range(2):
                        b = bits(src, h, g)
                        push = weight * along([wind[d, src, h, g] for d in range(3)], q)
                        state[h][g] = jnp.where(
                            (b & new_bit) != 0,
                            push,
                            jnp.where((b & prev_bit) != 0, 2.0 * BIG, fluid),
                        )
                state = pull(state, cy, cz)
                came = pull(
                    [[get(q, src, h, g) for g in range(2)] for h in range(2)], cy, cz
                )
                for h in halves:
                    for g in halves:
                        bounced = (
                            get(OPPOSITE[q], j, h, g) + state[h][g] * rho[h][g]
                        )
                        arrived = jnp.where(state[h][g] < 0.5 * BIG, bounced, came[h][g])
                        kept = jnp.where(uncovered[h, g], refill[h, g][q], arrived)
                        store(q, j, h, g, jnp.where(covered[h, g], get(q, j, h, g), kept))
                dens = pull([[get(RHO, src, h, g) for g in range(2)] for h in range(2)], cy, cz)
                term = 2.0 * came[0][0] - (weight * along(own, q)) * dens[0][0]
                linked = (state[0][0] > 0.5 * BIG) & (state[0][0] < 1.5 * BIG) & covered[0, 0]
                term = jnp.where(linked, term, 0.0)
                for d in range(3):
                    if VELOCITIES[q][d] == 1:
                        pushes[d] = pushes[d] + term
                    elif VELOCITIES[q][d] == -1:
                        pushes[d] = pushes[d] - term
            keep = jnp.logical_and(j >= 2, j <= 5)
            return tuple(jnp.where(keep, new, old) for new, old in zip(pushes, carry))

        zero = jnp.zeros((8, 128), F32)
        return lax.fori_loop(first, stop, plane, (zero, zero, zero))

    def get_first(f, j, h, g):
        return (ext_a, ext_b)[g][f, j, 8 * h : 8 * h + 8]

    def get_second(f, j, h, g):
        return post[f, j, h, g]

    def store_first(q, j, h, g, value):
        post[q, j, h, g] = value

    def store_second(q, j, h, g, value):
        fine_next[q, j - 2] = value

    first = substep(get_first, 1, 2, 1, 7, store_first, (0, 1))

    def relax(n, carry):
        j, h, g = 1 + n // 4, (n // 2) % 2, n % 2
        out, density = collided([post[q, j, h, g] for q in range(19)], FINE_RATE)
        for q in range(19):
            post[q, j, h, g] = out[q]
        post[RHO, j, h, g] = density
        return carry

    lax.fori_loop(0, 24, relax, 0)
    for edge, j in ((0, 1), (last, 6)):

        @pl.when(gx == edge)
        def _():
            for h in range(2):
                for g in range(2):
                    for f in range(20):
                        post[f, j, h, g] = get_first(f, j, h, g)

    second = substep(get_second, 2, 4, 2, 6, store_second, (0,))
    line = iota2((1, 128), 1)
    total = jnp.zeros((1, 128), F32)
    for n, value in enumerate(first + second):
        columns = jnp.sum(value, axis=0, keepdims=True)
        low = jnp.sum(jnp.where(line < 64, columns, 0.0), axis=1, keepdims=True)
        high = jnp.sum(jnp.where(line >= 64, columns, 0.0), axis=1, keepdims=True)
        at = n * 16 + 2 * gz
        total = jnp.where(line == at, low, jnp.where(line == at + 1, high, total))
    force[...] = jnp.broadcast_to(total, (8, 128))


def spread_kernel(got, out):
    out[...] = jnp.broadcast_to(jnp.sum(got[...], axis=0, keepdims=True), out.shape)


def boxes_kernel(got, out):
    b, r = iota2((16, 128), 0), iota2((16, 128), 1)
    pick = jnp.where(((b >> 2) == (r >> 5)) & ((b & 3) == ((r & 7) >> 1)), 1.0, 0.0)
    table = dot(pick, got[...])
    for n in range(6):
        rolled = pltpu.roll(table, (128 - 16 * n) % 128, 1) if n else table
        for bx in range(4):
            out[n // 3, n % 3, bx] = rolled[4 * bx : 4 * bx + 4, 0:16]


def call(kernel, shapes, operands, specs=None, scratch=(), name=None):
    return pl.pallas_call(
        kernel,
        out_shape=[jax.ShapeDtypeStruct(s, F32) for s in shapes],
        in_specs=specs or [VMEM] * len(operands),
        out_specs=[VMEM] * len(shapes),
        scratch_shapes=list(scratch),
        name=name,
    )(*operands)


def swapped(up, down, axis):
    count = lax.axis_size(axis)
    from_low = lax.ppermute(up, axis, [(i, (i + 1) % count) for i in range(count)])
    from_high = lax.ppermute(down, axis, [((i + 1) % count, i) for i in range(count)])
    return from_low, from_high


def shards(coarse_pdfs, fine_pdfs, centers, sphere_velocity):
    fp, cp, xr, xl = call(
        collide_kernel,
        ((20, 4, 8, 128), (19, 4, 8, 128), (30, 8, 128), (30, 8, 128)),
        (fine_pdfs, coarse_pdfs),
        name="collide",
    )
    code, wind = call(
        geometry_kernel,
        ((8, 2, 2, 8, 128), (3, 8, 2, 2, 8, 128)),
        (centers.reshape(-1), sphere_velocity.reshape(-1)),
        specs=[SMEM, SMEM],
        name="geometry",
    )
    r_l, r_r = swapped(xr, xl, GX)
    yr, yl = call(
        pack_y_kernel, ((31, 8, 128), (31, 8, 128)), (fp, cp, r_l, r_r), name="pack_y"
    )
    y_l, y_r = swapped(yr, yl, "gy")
    ext, cext, zr, zl = call(
        pack_z_kernel,
        ((20, 8, 16, 128), (19, 6, 8, 128), (8, 16, 128), (8, 16, 128)),
        (fp, cp, r_l, r_r, y_l, y_r),
        name="pack_z",
    )
    z_l, z_r = swapped(zr, zl, "gz")
    fine_next, coarse_next, force = call(
        main_kernel,
        (fine_pdfs.shape, coarse_pdfs.shape, (8, 128)),
        (ext, cext, z_l, z_r, code, wind),
        scratch=(
            pltpu.VMEM((20, 8, 16, 128), F32),
            pltpu.VMEM((20, 8, 2, 2, 8, 128), F32),
            pltpu.VMEM((4, 8, 2, 2, 8, 128), F32),
        ),
        name="main",
    )
    column = lax.all_to_all(force, "gz", 0, 0, tiled=True)
    (rows,) = call(spread_kernel, ((128, 128),), (column,), name="spread")
    rows = lax.all_to_all(rows, ("gx_0", "gx_1", "gy"), 0, 0, tiled=True)
    (sphere_force,) = call(boxes_kernel, ((2, 3, 4, 4, 16),), (rows,), name="boxes")
    return coarse_next, fine_next, sphere_force


def solution(mesh):
    split = Mesh(
        mesh.devices.reshape(8, 2, mesh.shape["gy"], mesh.shape["gz"]), ("gx_0", "gx_1", "gy", "gz")
    )
    return jax.shard_map(
        shards,
        mesh=split,
        in_specs=(P(None, GX, "gy", "gz"), P(None, GX, "gy", "gz"), P(), P()),
        out_specs=(P(None, GX, "gy", "gz"), P(None, GX, "gy", "gz"), P()),
        check_vma=False,
    )
```

```python
import jax
import jax.numpy as jnp
from jax import lax
from jax.experimental import pallas as pl
from jax.experimental.pallas import tpu as pltpu
from jax.sharding import Mesh
from jax.sharding import PartitionSpec as P

BOX_XY = 16
BOX_Z = 64
RADIUS = 4
GX = ("gx_0", "gx_1")
GY = ("gy_0", "gy_1")

VELOCITIES = (
    (0, 0, 0),
    (1, 0, 0),
    (-1, 0, 0),
    (0, 1, 0),
    (0, -1, 0),
    (0, 0, 1),
    (0, 0, -1),
    (1, 1, 0),
    (-1, -1, 0),
    (1, -1, 0),
    (-1, 1, 0),
    (1, 0, 1),
    (-1, 0, -1),
    (1, 0, -1),
    (-1, 0, 1),
    (0, 1, 1),
    (0, -1, -1),
    (0, 1, -1),
    (0, -1, 1),
)
OPPOSITE = (0, 2, 1, 4, 3, 6, 5, 8, 7, 10, 9, 12, 11, 14, 13, 16, 15, 18, 17)
WEIGHTS = (1.0 / 3.0,) + (1.0 / 18.0,) * 6 + (1.0 / 36.0,) * 12
COARSE_RATE = 1.25
FINE_RATE = 1.0 / 1.1
HIGHEST = lax.Precision.HIGHEST
RHO = 19
BIG = 1.0e30


def heading(axis, sign):
    return tuple(q for q in range(19) if VELOCITIES[q][axis] == sign)


XP, XM = heading(0, 1), heading(0, -1)
YP, YM = heading(1, 1), heading(1, -1)
ZP, ZM = heading(2, 1), heading(2, -1)
F32 = jnp.float32
VMEM = pl.BlockSpec(memory_space=pltpu.VMEM)
SMEM = pl.BlockSpec(memory_space=pltpu.SMEM)
ANY = pl.BlockSpec(memory_space=pl.ANY)


def along(vectors, q):
    total = None
    for d in range(3):
        sign = VELOCITIES[q][d]
        if sign == 0:
            continue
        if total is None:
            total = vectors[d] if sign == 1 else -vectors[d]
        else:
            total = total + vectors[d] if sign == 1 else total - vectors[d]
    return total


def equilibria(density, vectors):
    base = 1.0 - 1.5 * (
        vectors[0] * vectors[0] + vectors[1] * vectors[1] + vectors[2] * vectors[2]
    )
    scaled = {w: w * density for w in set(WEIGHTS)}
    out = [scaled[WEIGHTS[0]] * base]
    for q in range(1, 19, 2):
        c = along(vectors, q)
        even = base + 4.5 * c * c
        odd = 3.0 * c
        out.append(scaled[WEIGHTS[q]] * (even + odd))
        out.append(scaled[WEIGHTS[q]] * (even - odd))
    return out


def collided(p, rate):
    density = p[0]
    for q in range(1, 19):
        density = density + p[q]
    inverse = 1.0 / density
    vectors = []
    for d in range(3):
        total = None
        for q in range(19):
            sign = VELOCITIES[q][d]
            if sign == 1:
                total = p[q] if total is None else total + p[q]
        for q in range(19):
            if VELOCITIES[q][d] == -1:
                total = total - p[q]
        vectors.append(total * inverse)
    targets = equilibria(density, vectors)
    return [p[q] - rate * (p[q] - targets[q]) for q in range(19)], density


def dot(a, b):
    return lax.dot_general(
        a, b, (((1,), (0,)), ((), ())), precision=HIGHEST, preferred_element_type=F32
    )


def iota2(shape, axis):
    return lax.broadcasted_iota(jnp.int32, shape, axis)


def upsampled(tiles):
    rows = tiles.shape[0]
    r, c = iota2((rows, rows), 0), iota2((rows, rows), 1)
    left = jnp.where(((r >> 3) == (c >> 3)) & (((r & 7) >> 1) == (c & 7)), 1.0, 0.0)
    k, n = iota2((128, 128), 0), iota2((128, 128), 1)
    right = jnp.where(k == (n >> 1), 1.0, 0.0)
    return dot(left, dot(tiles, right))


def coalesced(tiles):
    rows = tiles.shape[0]
    r, c = iota2((rows, rows), 0), iota2((rows, rows), 1)
    left = jnp.where(((r >> 3) == (c >> 3)) & ((r & 7) == ((c & 7) >> 1)), 0.25, 0.0)
    k, n = iota2((128, 128), 0), iota2((128, 128), 1)
    right = jnp.where((k >> 1) == n, 1.0, 0.0)
    return dot(left, dot(tiles, right))


def collide_kernel(fine, coarse, fp, cp, xr, xl):
    gx = lax.axis_index(GX)
    last = lax.axis_size(GX) - 1
    cp[...] = jnp.zeros(cp.shape, F32)
    for x in range(4):
        post, density = collided([coarse[q, x] for q in range(19)], COARSE_RATE)
        for q in range(19):
            cp[q, x, 0:4, 0:64] = post[q]

    def plane(x, carry):
        post, density = collided([fine[q, x] for q in range(19)], FINE_RATE)
        for q in range(19):
            fp[q, x] = post[q]
        fp[RHO, x] = density
        return carry

    lax.fori_loop(0, 4, plane, 0)
    for out, near, far, inward, edge in ((xr, 3, 2, XP, last), (xl, 0, 1, XM, 0)):
        for k, q in enumerate(inward):
            out[19 + k] = fp[q, far]
        out[24] = fp[RHO, far]

        @pl.when(gx != edge)
        def _():
            out[0:19] = fp[0:19, near]
            for k, q in enumerate(inward):
                out[25 + k] = cp[q, near]

        @pl.when(gx == edge)
        def _():
            up = upsampled(cp[:, near].reshape(152, 128))
            out[0:19] = up.reshape(19, 8, 128)
            picked = jnp.concatenate([fp[q, near] for q in inward], axis=0)
            out[25:30] = coalesced(picked).reshape(5, 8, 128)


def pack_y_kernel(fp, cp, r_l, r_r, after, yr, yl):
    rho_l, rho_r = r_l[0], r_r[0]
    for q in range(1, 19):
        rho_l = rho_l + r_l[q]
        rho_r = rho_r + r_r[q]
    for out, near, far, cnear, inward in ((yr, 7, 6, 3, YP), (yl, 0, 1, 0, YM)):
        out[...] = jnp.zeros(out.shape, F32)
        out[0:19, 1:2] = r_l[0:19, near : near + 1]
        out[RHO, 1:2] = rho_l[near : near + 1]
        out[0:19, 6:7] = r_r[0:19, near : near + 1]
        out[RHO, 6:7] = rho_r[near : near + 1]
        for x in range(4):
            out[0:20, 2 + x : 3 + x] = fp[:, x, near : near + 1]
        for k in range(5):
            out[XP[k], 0:1] = r_l[19 + k, near : near + 1]
            out[XM[k], 7:8] = r_r[19 + k, near : near + 1]
        out[RHO, 0:1] = r_l[24, near : near + 1]
        out[RHO, 7:8] = r_r[24, near : near + 1]
        for k, q in enumerate(inward):
            out[20 + k, 1:2] = r_l[q, far : far + 1]
            out[20 + k, 6:7] = r_r[q, far : far + 1]
            for x in range(4):
                out[20 + k, 2 + x : 3 + x] = fp[q, x, far : far + 1]
                out[26 + k, 1 + x : 2 + x] = cp[q, x, cnear : cnear + 1]
            if q in XP:
                out[20 + k, 0:1] = r_l[19 + XP.index(q), far : far + 1]
                out[26 + k, 0:1] = r_l[25 + XP.index(q), cnear : cnear + 1]
            if q in XM:
                out[20 + k, 7:8] = r_r[19 + XM.index(q), far : far + 1]
                out[26 + k, 5:6] = r_r[25 + XM.index(q), cnear : cnear + 1]
        out[25, 0:1] = r_l[24, far : far + 1]
        out[25, 1:2] = rho_l[far : far + 1]
        out[25, 6:7] = rho_r[far : far + 1]
        out[25, 7:8] = r_r[24, far : far + 1]
        for x in range(4):
            out[25, 2 + x : 3 + x] = fp[RHO, x, far : far + 1]


def pack_z_kernel(fp, cp, r_l, r_r, y_l, y_r, ext, cext, zr, zl):
    for x in range(4):
        ext[:, 2 + x, 0:8] = fp[:, x]
        cext[:, 1 + x] = cp[:, x]
    cext[:, 0] = jnp.zeros((19, 8, 128), F32)
    cext[:, 5] = jnp.zeros((19, 8, 128), F32)
    for got, near, far, cplane, inward in ((r_l, 1, 0, 0, XP), (r_r, 6, 7, 5, XM)):
        ext[0:19, near, 0:8] = got[0:19]
        density = got[0]
        for q in range(1, 19):
            density = density + got[q]
        ext[RHO, near, 0:8] = density
        for k, q in enumerate(inward):
            ext[q, far, 0:8] = got[19 + k]
            cext[q, cplane] = got[25 + k]
        ext[RHO, far, 0:8] = got[24]
    for j in range(8):
        for got, near, far, crow, inward in ((y_l, 15, 14, 7, YP), (y_r, 8, 9, 4, YM)):
            ext[:, j, near : near + 1] = got[0:20, j : j + 1]
            for k, q in enumerate(inward):
                ext[q, j, far : far + 1] = got[20 + k, j : j + 1]
                if j < 6:
                    cext[q, j, crow : crow + 1] = got[26 + k, j : j + 1]
            ext[RHO, j, far : far + 1] = got[25, j : j + 1]
    lane = iota2((8, 128), 1)

    def plane(j, carry):
        for h in range(2):
            to_r = jnp.zeros((8, 128), F32)
            to_l = jnp.zeros((8, 128), F32)
            for f in range(20):
                turned = pltpu.roll(ext[f, j, 8 * h : 8 * h + 8], (2 * f + 2) % 128, 1)
                to_r = jnp.where((lane >> 1) == f, turned, to_r)
                to_l = jnp.where((lane >> 1) == f + 1, turned, to_l)
            if h == 0:
                jc = jnp.minimum(j, 5)
                for k in range(5):
                    to_r = jnp.where(lane == 64 + k, pltpu.roll(cext[ZP[k], jc], k + 1, 1), to_r)
                    to_l = jnp.where(lane == 64 + k, pltpu.roll(cext[ZM[k], jc], 64 + k, 1), to_l)
            zr[j, 8 * h : 8 * h + 8] = to_r
            zl[j, 8 * h : 8 * h + 8] = to_l
        return carry

    lax.fori_loop(0, 8, plane, 0)


def geometry_kernel(centers, velocity, after, code, wind):
    gx, gy, gz = lax.axis_index(GX), lax.axis_index(GY), lax.axis_index("gz")
    row, lane = iota2((8, 128), 0), iota2((8, 128), 1)
    low_row, low_lane = row < 4, lane < 64
    nbx, nby, nbz = 4, 4, 16
    boxes = nbx * nby * nbz
    y0, z0, x0 = gy * 8, gz * 128, gx * 4
    own_y = y0 // BOX_XY
    prev_y = lax.rem(lax.div(y0 + nby * BOX_XY - 1, BOX_XY), nby)
    next_y = lax.rem(lax.div(y0 + 8, BOX_XY), nby)
    lo_z = z0 // BOX_Z
    prev_z = lax.rem(lo_z + nbz - 1, nbz)
    next_z = lax.rem(lo_z + 2, nbz)
    row_boxes = ((own_y, own_y), (next_y, prev_y))
    lane_boxes = ((lo_z, lo_z + 1), (next_z, prev_z))
    y_of = (row, jnp.where(low_row, row + 8, row - 8))
    z_of = (lane, jnp.where(low_lane, lane + 128, lane - 128))
    off_y = [((y0 + y_of[h] + BOX_XY * nby) & (BOX_XY - 1)).astype(F32) for h in range(2)]
    off_z = [((z0 + z_of[h] + BOX_Z * nbz) & (BOX_Z - 1)).astype(F32) for h in range(2)]

    def plane(j, carry):
        x = x0 + j - 2
        inside = jnp.where((x >= 0) & (x < nbx * BOX_XY), 1.0, 0.0)
        safe = jnp.clip(x, 0, nbx * BOX_XY - 1)
        bx = lax.div(safe, BOX_XY)
        off_x = lax.rem(safe, BOX_XY).astype(F32)

        def field(table, base, h, g):
            def one(by, bz):
                return table[base + (bx * nby + by) * nbz + bz].astype(F32)

            upper = jnp.where(
                low_lane,
                one(row_boxes[h][0], lane_boxes[g][0]),
                one(row_boxes[h][0], lane_boxes[g][1]),
            )
            if h == 0:
                return upper
            lower = jnp.where(
                low_lane,
                one(row_boxes[h][1], lane_boxes[g][0]),
                one(row_boxes[h][1], lane_boxes[g][1]),
            )
            return jnp.where(low_row, upper, lower)

        for h in range(2):
            for g in range(2):
                bits = jnp.zeros((8, 128), F32)
                for moment in range(3):
                    base = moment * 3 * boxes
                    gap_x = off_x - field(centers, base, h, g)
                    gap_y = off_y[h] - field(centers, base + boxes, h, g)
                    gap_z = off_z[g] - field(centers, base + 2 * boxes, h, g)
                    distance = gap_x * gap_x + gap_y * gap_y + gap_z * gap_z
                    hit = (distance <= float(RADIUS * RADIUS)) & (inside > 0.5)
                    bits = bits + jnp.where(hit, float(1 << moment), 0.0)
                code[j, h, g] = bits
                for d in range(3):
                    wind[d, j, h, g] = field(velocity, d * boxes, h, g) * inside
        return carry

    lax.fori_loop(0, 8, plane, 0)


def turned(tiles, step, axis):
    size = 8 if axis == 0 else 128
    at = iota2((8, 128), axis)
    rolled = [pltpu.roll(t, step % size, axis) for t in tiles]
    seam = at == (0 if step == 1 else size - 1)
    return [jnp.where(seam, rolled[1], rolled[0]), jnp.where(seam, rolled[0], rolled[1])]


def pull(tiles, cy, cz):
    if cz:
        tiles = [turned(tiles[h], cz, 1) for h in range(2)]
    if cy:
        first = turned([tiles[0][0], tiles[1][0]], cy, 0)
        second = turned([tiles[0][1], tiles[1][1]], cy, 0)
        tiles = [[first[0], second[0]], [first[1], second[1]]]
    return tiles


def main_kernel(ext_a, cext, z_l, z_r, code, wind, fine_next, coarse_next, force, ext_b, post, sums):
    gx, gz = lax.axis_index(GX), lax.axis_index("gz")
    last = lax.axis_size(GX) - 1
    row, lane = iota2((8, 128), 0), iota2((8, 128), 1)

    for k in range(5):
        q = ZP[k]
        for x in range(4):
            j = 1 + x - VELOCITIES[q][0]
            tile = jnp.where(lane == 127, pltpu.roll(z_l[j, 0:8], 63 - k, 1), cext[q, j])
            tile = pltpu.roll(tile, 1, 1)
            if VELOCITIES[q][1]:
                tile = pltpu.roll(tile, VELOCITIES[q][1] % 8, 0)
            coarse_next[q, x] = tile[0:4, 0:64]
        q = ZM[k]
        for x in range(4):
            j = 1 + x - VELOCITIES[q][0]
            tile = z_r[j, 0:8]
            if k:
                tile = pltpu.roll(tile, 128 - k, 1)
            tile = jnp.where(lane == 64, tile, cext[q, j])
            tile = pltpu.roll(tile, 127, 1)
            if VELOCITIES[q][1]:
                tile = pltpu.roll(tile, VELOCITIES[q][1] % 8, 0)
            coarse_next[q, x] = tile[0:4, 0:64]
    for q in range(19):
        if VELOCITIES[q][2] == 0:
            for x in range(4):
                tile = cext[q, 1 + x - VELOCITIES[q][0]]
                if VELOCITIES[q][1]:
                    tile = pltpu.roll(tile, VELOCITIES[q][1] % 8, 0)
                coarse_next[q, x] = tile[0:4, 0:64]

    def unpack(j, carry):
        for h in range(2):
            from_l = z_l[j, 8 * h : 8 * h + 8]
            from_r = z_r[j, 8 * h : 8 * h + 8]
            for f in range(20):
                before = pltpu.roll(from_l, (126 - 2 * f) % 128, 1)
                after = pltpu.roll(from_r, (126 - 2 * f) % 128, 1)
                ext_b[f, j, 8 * h : 8 * h + 8] = jnp.where(lane < 64, after, before)
        return carry

    lax.fori_loop(0, 8, unpack, 0)

    def substep(get, prev_bit, new_bit, first, stop, store, halves):
        def bits(j, h, g):
            return code[j, h, g].astype(jnp.int32)

        def prepare(j, carry):
            rho_open, open_ = [[None] * 2, [None] * 2], [[None] * 2, [None] * 2]
            for h in range(2):
                for g in range(2):
                    is_open = (bits(j, h, g) & (prev_bit | new_bit)) == 0
                    open_[h][g] = jnp.where(is_open, 1.0, 0.0)
                    rho_open[h][g] = jnp.where(is_open, get(RHO, j, h, g), 0.0)
            for n, tiles in enumerate((rho_open, open_)):
                back, forth = pull(tiles, 0, 1), pull(tiles, 0, -1)
                side_z = [[back[h][g] + forth[h][g] for g in range(2)] for h in range(2)]
                down, up = pull(tiles, 1, 0), pull(tiles, -1, 0)
                down2, up2 = pull(side_z, 1, 0), pull(side_z, -1, 0)
                for h in halves:
                    for g in halves:
                        side_y = down[h][g] + up[h][g]
                        both = down2[h][g] + up2[h][g]
                        sums[2 * n, j, h, g] = 2.0 * (side_y + side_z[h][g]) + both
                        sums[2 * n + 1, j, h, g] = 2.0 * tiles[h][g] + side_y + side_z[h][g]
            return carry

        lax.fori_loop(first - 1, stop + 1, prepare, 0)

        def plane(j, carry):
            pushes = list(carry)
            mine = [[bits(j, h, g) for g in range(2)] for h in range(2)]
            rho = [[get(RHO, j, h, g) for g in range(2)] for h in range(2)]
            covered, uncovered, refill = {}, {}, {}
            for h in halves:
                for g in halves:
                    covered[h, g] = (mine[h][g] & new_bit) != 0
                    uncovered[h, g] = (mine[h][g] & prev_bit) != 0
                    above = (
                        12.0 * rho[h][g]
                        + sums[0, j, h, g]
                        + (sums[1, j - 1, h, g] + sums[1, j + 1, h, g])
                    )
                    below = 12.0 + sums[2, j, h, g] + (sums[3, j - 1, h, g] + sums[3, j + 1, h, g])
                    density = above / below
                    own = [wind[d, j, h, g] for d in range(3)]
                    refill[h, g] = equilibria(density, own)
            own = [wind[d, j, 0, 0] for d in range(3)]
            for q in range(19):
                cx, cy, cz = VELOCITIES[q]
                weight = 6.0 * WEIGHTS[q]
                if q == 0:
                    for h in halves:
                        for g in halves:
                            p0 = get(0, j, h, g)
                            kept = jnp.where(uncovered[h, g], refill[h, g][0], p0)
                            store(0, j, h, g, jnp.where(covered[h, g], p0, kept))
                    continue
                src = j - cx
                ghost = jnp.logical_or(
                    jnp.logical_and(gx == 0, src < 2), jnp.logical_and(gx == last, src > 5)
                )
                fluid = jnp.where(ghost, 2.0 * BIG, BIG)
                state = [[None] * 2, [None] * 2]
                for h in range(2):
                    for g in range(2):
                        b = bits(src, h, g)
                        push = weight * along([wind[d, src, h, g] for d in range(3)], q)
                        state[h][g] = jnp.where(
                            (b & new_bit) != 0,
                            push,
                            jnp.where((b & prev_bit) != 0, 2.0 * BIG, fluid),
                        )
                state = pull(state, cy, cz)
                came = pull(
                    [[get(q, src, h, g) for g in range(2)] for h in range(2)], cy, cz
                )
                for h in halves:
                    for g in halves:
                        bounced = (
                            get(OPPOSITE[q], j, h, g) + state[h][g] * rho[h][g]
                        )
                        arrived = jnp.where(state[h][g] < 0.5 * BIG, bounced, came[h][g])
                        kept = jnp.where(uncovered[h, g], refill[h, g][q], arrived)
                        store(q, j, h, g, jnp.where(covered[h, g], get(q, j, h, g), kept))
                dens = pull([[get(RHO, src, h, g) for g in range(2)] for h in range(2)], cy, cz)
                term = 2.0 * came[0][0] - (weight * along(own, q)) * dens[0][0]
                linked = (state[0][0] > 0.5 * BIG) & (state[0][0] < 1.5 * BIG) & covered[0, 0]
                term = jnp.where(linked, term, 0.0)
                for d in range(3):
                    if VELOCITIES[q][d] == 1:
                        pushes[d] = pushes[d] + term
                    elif VELOCITIES[q][d] == -1:
                        pushes[d] = pushes[d] - term
            keep = jnp.logical_and(j >= 2, j <= 5)
            return tuple(jnp.where(keep, new, old) for new, old in zip(pushes, carry))

        zero = jnp.zeros((8, 128), F32)
        return lax.fori_loop(first, stop, plane, (zero, zero, zero))

    def get_first(f, j, h, g):
        return (ext_a, ext_b)[g][f, j, 8 * h : 8 * h + 8]

    def get_second(f, j, h, g):
        return post[f, j, h, g]

    def store_first(q, j, h, g, value):
        post[q, j, h, g] = value

    def store_second(q, j, h, g, value):
        fine_next[q, j - 2] = value

    first = substep(get_first, 1, 2, 1, 7, store_first, (0, 1))

    def relax(n, carry):
        j, h, g = 1 + n // 4, (n // 2) % 2, n % 2
        out, density = collided([post[q, j, h, g] for q in range(19)], FINE_RATE)
        for q in range(19):
            post[q, j, h, g] = out[q]
        post[RHO, j, h, g] = density
        return carry

    lax.fori_loop(0, 24, relax, 0)
    for edge, j in ((0, 1), (last, 6)):

        @pl.when(gx == edge)
        def _():
            for h in range(2):
                for g in range(2):
                    for f in range(20):
                        post[f, j, h, g] = get_first(f, j, h, g)

    second = substep(get_second, 2, 4, 2, 6, store_second, (0,))
    line = iota2((1, 128), 1)
    total = jnp.zeros((1, 128), F32)
    for n, value in enumerate(first + second):
        columns = jnp.sum(value, axis=0, keepdims=True)
        low = jnp.sum(jnp.where(line < 64, columns, 0.0), axis=1, keepdims=True)
        high = jnp.sum(jnp.where(line >= 64, columns, 0.0), axis=1, keepdims=True)
        at = n * 16 + 2 * gz
        total = jnp.where(line == at, low, jnp.where(line == at + 1, high, total))
    force[...] = jnp.broadcast_to(total, (32, 128))


def spread_kernel(got, out):
    out[...] = jnp.broadcast_to(jnp.sum(got[...], axis=0, keepdims=True), out.shape)


def boxes_kernel(got, out):
    b, r = iota2((16, 32), 0), iota2((16, 32), 1)
    pick = jnp.where(((b >> 2) == (r >> 3)) & ((b & 3) == (r & 3)), 1.0, 0.0)
    table = dot(pick, got[...])
    for n in range(6):
        rolled = pltpu.roll(table, (128 - 16 * n) % 128, 1) if n else table
        for bx in range(4):
            out[n // 3, n % 3, bx] = rolled[4 * bx : 4 * bx + 4, 0:16]


def call(kernel, shapes, operands, specs=None, scratch=(), name=None, keep=True, near=None):
    near = [s is not SMEM for s in specs or [VMEM] * len(operands)] if near is None else near
    operands = [
        pltpu.with_memory_space_constraint(x, pltpu.VMEM) if n else x
        for x, n in zip(operands, near)
    ]
    return pl.pallas_call(
        kernel,
        out_shape=[(pltpu.VMEM if keep else jax.ShapeDtypeStruct)(s, F32) for s in shapes],
        in_specs=specs or [VMEM] * len(operands),
        out_specs=[VMEM] * len(shapes),
        scratch_shapes=list(scratch),
        compiler_params=pltpu.CompilerParams(vmem_limit_bytes=24 * 2**20),
        name=name,
    )(*operands)


def swapped(up, down, axis):
    count = lax.axis_size(axis)
    from_low = lax.ppermute(up, axis, [(i, (i + 1) % count) for i in range(count)])
    from_high = lax.ppermute(down, axis, [((i + 1) % count, i) for i in range(count)])
    return from_low, from_high


def shards(coarse_pdfs, fine_pdfs, centers, sphere_velocity):
    fp, cp, xr, xl = call(
        collide_kernel,
        ((20, 4, 8, 128), (19, 4, 8, 128), (30, 8, 128), (30, 8, 128)),
        (fine_pdfs, coarse_pdfs),
        near=[False] * 2,
        name="collide",
    )
    code, wind = call(
        geometry_kernel,
        ((8, 2, 2, 8, 128), (3, 8, 2, 2, 8, 128)),
        (centers.reshape(-1), sphere_velocity.reshape(-1), xr),
        specs=[SMEM, SMEM, ANY],
        name="geometry",
    )
    r_l, r_r = swapped(xr, xl, GX)
    yr, yl = call(
        pack_y_kernel,
        ((31, 8, 128), (31, 8, 128)),
        (fp, cp, r_l, r_r, code),
        specs=[VMEM] * 4 + [ANY],
        name="pack_y",
    )
    y_l, y_r = swapped(yr, yl, GY)
    ext, cext, zr, zl = call(
        pack_z_kernel,
        ((20, 8, 16, 128), (19, 6, 8, 128), (8, 16, 128), (8, 16, 128)),
        (fp, cp, r_l, r_r, y_l, y_r),
        name="pack_z",
    )
    z_l, z_r = swapped(zr, zl, "gz")
    fine_next, coarse_next, force = call(
        main_kernel,
        (fine_pdfs.shape, coarse_pdfs.shape, (32, 128)),
        (ext, cext, z_l, z_r, code, wind),
        keep=False,
        scratch=(
            pltpu.VMEM((20, 8, 16, 128), F32),
            pltpu.VMEM((20, 8, 2, 2, 8, 128), F32),
            pltpu.VMEM((4, 8, 2, 2, 8, 128), F32),
        ),
        name="main",
    )
    column = lax.all_to_all(force, ("gx_1", "gy_1", "gz"), 0, 0, tiled=True)
    (rows,) = call(spread_kernel, ((32, 128),), (column,), near=[False], name="spread", keep=False)
    rows = lax.all_to_all(rows, ("gx_0", "gy_0"), 0, 0, tiled=True)
    (sphere_force,) = call(boxes_kernel, ((2, 3, 4, 4, 16),), (rows,), near=[False], name="boxes", keep=False)
    return coarse_next, fine_next, sphere_force


def solution(mesh):
    split = Mesh(
        mesh.devices.reshape(8, 2, 4, 2, mesh.shape["gz"]), ("gx_0", "gx_1", "gy_0", "gy_1", "gz")
    )
    return jax.shard_map(
        shards,
        mesh=split,
        in_specs=(P(None, GX, GY, "gz"), P(None, GX, GY, "gz"), P(), P()),
        out_specs=(P(None, GX, GY, "gz"), P(None, GX, GY, "gz"), P()),
        check_vma=False,
    )
```

```python
import jax
import jax.numpy as jnp
from jax import lax
from jax.experimental import pallas as pl
from jax.experimental.pallas import tpu as pltpu
from jax.sharding import Mesh
from jax.sharding import PartitionSpec as P

BOX_XY = 16
BOX_Z = 64
RADIUS = 4
GX = ("gx_0", "gx_1")
GY = ("gy_0", "gy_1")

VELOCITIES = (
    (0, 0, 0),
    (1, 0, 0),
    (-1, 0, 0),
    (0, 1, 0),
    (0, -1, 0),
    (0, 0, 1),
    (0, 0, -1),
    (1, 1, 0),
    (-1, -1, 0),
    (1, -1, 0),
    (-1, 1, 0),
    (1, 0, 1),
    (-1, 0, -1),
    (1, 0, -1),
    (-1, 0, 1),
    (0, 1, 1),
    (0, -1, -1),
    (0, 1, -1),
    (0, -1, 1),
)
OPPOSITE = (0, 2, 1, 4, 3, 6, 5, 8, 7, 10, 9, 12, 11, 14, 13, 16, 15, 18, 17)
WEIGHTS = (1.0 / 3.0,) + (1.0 / 18.0,) * 6 + (1.0 / 36.0,) * 12
COARSE_RATE = 1.25
FINE_RATE = 1.0 / 1.1
HIGHEST = lax.Precision.HIGHEST
RHO = 19
BIG = 1.0e30


def heading(axis, sign):
    return tuple(q for q in range(19) if VELOCITIES[q][axis] == sign)


XP, XM = heading(0, 1), heading(0, -1)
YP, YM = heading(1, 1), heading(1, -1)
ZP, ZM = heading(2, 1), heading(2, -1)
F32 = jnp.float32
VMEM = pl.BlockSpec(memory_space=pltpu.VMEM)
SMEM = pl.BlockSpec(memory_space=pltpu.SMEM)
ANY = pl.BlockSpec(memory_space=pl.ANY)


def along(vectors, q):
    total = None
    for d in range(3):
        sign = VELOCITIES[q][d]
        if sign == 0:
            continue
        if total is None:
            total = vectors[d] if sign == 1 else -vectors[d]
        else:
            total = total + vectors[d] if sign == 1 else total - vectors[d]
    return total


def equilibria(density, vectors):
    base = 1.0 - 1.5 * (
        vectors[0] * vectors[0] + vectors[1] * vectors[1] + vectors[2] * vectors[2]
    )
    scaled = {w: w * density for w in set(WEIGHTS)}
    out = [scaled[WEIGHTS[0]] * base]
    for q in range(1, 19, 2):
        c = along(vectors, q)
        even = base + 4.5 * c * c
        odd = 3.0 * c
        out.append(scaled[WEIGHTS[q]] * (even + odd))
        out.append(scaled[WEIGHTS[q]] * (even - odd))
    return out


def collided(p, rate):
    density = p[0]
    for q in range(1, 19):
        density = density + p[q]
    inverse = 1.0 / density
    vectors = []
    for d in range(3):
        total = None
        for q in range(19):
            sign = VELOCITIES[q][d]
            if sign == 1:
                total = p[q] if total is None else total + p[q]
        for q in range(19):
            if VELOCITIES[q][d] == -1:
                total = total - p[q]
        vectors.append(total * inverse)
    targets = equilibria(density, vectors)
    return [p[q] - rate * (p[q] - targets[q]) for q in range(19)], density


def dot(a, b):
    return lax.dot_general(
        a, b, (((1,), (0,)), ((), ())), precision=HIGHEST, preferred_element_type=F32
    )


def iota2(shape, axis):
    return lax.broadcasted_iota(jnp.int32, shape, axis)


def upsampled(tiles):
    rows = tiles.shape[0]
    r, c = iota2((rows, rows), 0), iota2((rows, rows), 1)
    left = jnp.where(((r >> 3) == (c >> 3)) & (((r & 7) >> 1) == (c & 7)), 1.0, 0.0)
    k, n = iota2((128, 128), 0), iota2((128, 128), 1)
    right = jnp.where(k == (n >> 1), 1.0, 0.0)
    return dot(left, dot(tiles, right))


def coalesced(tiles):
    rows = tiles.shape[0]
    r, c = iota2((rows, rows), 0), iota2((rows, rows), 1)
    left = jnp.where(((r >> 3) == (c >> 3)) & ((r & 7) == ((c & 7) >> 1)), 0.25, 0.0)
    k, n = iota2((128, 128), 0), iota2((128, 128), 1)
    right = jnp.where((k >> 1) == n, 1.0, 0.0)
    return dot(left, dot(tiles, right))


def collide_kernel(fine_in, coarse_in, fp, cp, xr, xl, fine, coarse, sems):
    bring_coarse = pltpu.make_async_copy(coarse_in, coarse, sems.at[0])
    bring_fine = pltpu.make_async_copy(fine_in, fine, sems.at[1])
    bring_fine.start()
    bring_coarse.start()
    gx = lax.axis_index(GX)
    last = lax.axis_size(GX) - 1
    cp[...] = jnp.zeros(cp.shape, F32)
    bring_coarse.wait()
    for x in range(4):
        post, density = collided([coarse[q, x] for q in range(19)], COARSE_RATE)
        for q in range(19):
            cp[q, x, 0:4, 0:64] = post[q]

    bring_fine.wait()

    def plane(x, carry):
        post, density = collided([fine[q, x] for q in range(19)], FINE_RATE)
        for q in range(19):
            fp[q, x] = post[q]
        fp[RHO, x] = density
        return carry

    lax.fori_loop(0, 4, plane, 0)
    for out, near, far, inward, edge in ((xr, 3, 2, XP, last), (xl, 0, 1, XM, 0)):
        for k, q in enumerate(inward):
            out[19 + k] = fp[q, far]
        out[24] = fp[RHO, far]

        @pl.when(gx != edge)
        def _():
            out[0:19] = fp[0:19, near]
            for k, q in enumerate(inward):
                out[25 + k] = cp[q, near]

        @pl.when(gx == edge)
        def _():
            up = upsampled(cp[:, near].reshape(152, 128))
            out[0:19] = up.reshape(19, 8, 128)
            picked = jnp.concatenate([fp[q, near] for q in inward], axis=0)
            out[25:30] = coalesced(picked).reshape(5, 8, 128)


def pack_y_kernel(fp, cp, r_l, r_r, after, yr, yl):
    rho_l, rho_r = r_l[0], r_r[0]
    for q in range(1, 19):
        rho_l = rho_l + r_l[q]
        rho_r = rho_r + r_r[q]
    for out, near, far, cnear, inward in ((yr, 7, 6, 3, YP), (yl, 0, 1, 0, YM)):
        out[...] = jnp.zeros(out.shape, F32)
        out[0:19, 1:2] = r_l[0:19, near : near + 1]
        out[RHO, 1:2] = rho_l[near : near + 1]
        out[0:19, 6:7] = r_r[0:19, near : near + 1]
        out[RHO, 6:7] = rho_r[near : near + 1]
        for x in range(4):
            out[0:20, 2 + x : 3 + x] = fp[:, x, near : near + 1]
        for k in range(5):
            out[XP[k], 0:1] = r_l[19 + k, near : near + 1]
            out[XM[k], 7:8] = r_r[19 + k, near : near + 1]
        out[RHO, 0:1] = r_l[24, near : near + 1]
        out[RHO, 7:8] = r_r[24, near : near + 1]
        for k, q in enumerate(inward):
            out[20 + k, 1:2] = r_l[q, far : far + 1]
            out[20 + k, 6:7] = r_r[q, far : far + 1]
            for x in range(4):
                out[20 + k, 2 + x : 3 + x] = fp[q, x, far : far + 1]
                out[26 + k, 1 + x : 2 + x] = cp[q, x, cnear : cnear + 1]
            if q in XP:
                out[20 + k, 0:1] = r_l[19 + XP.index(q), far : far + 1]
                out[26 + k, 0:1] = r_l[25 + XP.index(q), cnear : cnear + 1]
            if q in XM:
                out[20 + k, 7:8] = r_r[19 + XM.index(q), far : far + 1]
                out[26 + k, 5:6] = r_r[25 + XM.index(q), cnear : cnear + 1]
        out[25, 0:1] = r_l[24, far : far + 1]
        out[25, 1:2] = rho_l[far : far + 1]
        out[25, 6:7] = rho_r[far : far + 1]
        out[25, 7:8] = r_r[24, far : far + 1]
        for x in range(4):
            out[25, 2 + x : 3 + x] = fp[RHO, x, far : far + 1]


def pack_z_kernel(fp, cp, r_l, r_r, y_l, y_r, ext, cext, zr, zl):
    for x in range(4):
        ext[:, 2 + x, 0:8] = fp[:, x]
        cext[:, 1 + x] = cp[:, x]
    cext[:, 0] = jnp.zeros((19, 8, 128), F32)
    cext[:, 5] = jnp.zeros((19, 8, 128), F32)
    for got, near, far, cplane, inward in ((r_l, 1, 0, 0, XP), (r_r, 6, 7, 5, XM)):
        ext[0:19, near, 0:8] = got[0:19]
        density = got[0]
        for q in range(1, 19):
            density = density + got[q]
        ext[RHO, near, 0:8] = density
        for k, q in enumerate(inward):
            ext[q, far, 0:8] = got[19 + k]
            cext[q, cplane] = got[25 + k]
        ext[RHO, far, 0:8] = got[24]
    for j in range(8):
        for got, near, far, crow, inward in ((y_l, 15, 14, 7, YP), (y_r, 8, 9, 4, YM)):
            ext[:, j, near : near + 1] = got[0:20, j : j + 1]
            for k, q in enumerate(inward):
                ext[q, j, far : far + 1] = got[20 + k, j : j + 1]
                if j < 6:
                    cext[q, j, crow : crow + 1] = got[26 + k, j : j + 1]
            ext[RHO, j, far : far + 1] = got[25, j : j + 1]
    lane = iota2((8, 128), 1)

    def plane(j, carry):
        for h in range(2):
            to_r = jnp.zeros((8, 128), F32)
            to_l = jnp.zeros((8, 128), F32)
            for f in range(20):
                turned = pltpu.roll(ext[f, j, 8 * h : 8 * h + 8], (4 * f + 2) % 128, 1)
                to_r = jnp.where((lane >> 1) == 2 * f, turned, to_r)
                to_l = jnp.where((lane >> 1) == 2 * f + 1, turned, to_l)
            if h == 0:
                jc = jnp.minimum(j, 5)
                for k in range(5):
                    to_r = jnp.where(lane == 96 + k, pltpu.roll(cext[ZP[k], jc], 33 + k, 1), to_r)
                    to_l = jnp.where(lane == 96 + k, pltpu.roll(cext[ZM[k], jc], 96 + k, 1), to_l)
            zr[j, 8 * h : 8 * h + 8] = to_r
            zl[j, 8 * h : 8 * h + 8] = to_l
        return carry

    lax.fori_loop(0, 8, plane, 0)


def geometry_kernel(centers, velocity, after, code, wind):
    gx, gy, gz = lax.axis_index(GX), lax.axis_index(GY), lax.axis_index("gz")
    row, lane = iota2((8, 128), 0), iota2((8, 128), 1)
    low_row, low_lane = row < 4, lane < 64
    nbx, nby, nbz = 4, 4, 16
    boxes = nbx * nby * nbz
    y0, z0, x0 = gy * 8, gz * 128, gx * 4
    own_y = y0 // BOX_XY
    prev_y = lax.rem(lax.div(y0 + nby * BOX_XY - 1, BOX_XY), nby)
    next_y = lax.rem(lax.div(y0 + 8, BOX_XY), nby)
    lo_z = z0 // BOX_Z
    prev_z = lax.rem(lo_z + nbz - 1, nbz)
    next_z = lax.rem(lo_z + 2, nbz)
    row_boxes = ((own_y, own_y), (next_y, prev_y))
    lane_boxes = ((lo_z, lo_z + 1), (next_z, prev_z))
    y_of = (row, jnp.where(low_row, row + 8, row - 8))
    z_of = (lane, jnp.where(low_lane, lane + 128, lane - 128))
    off_y = [((y0 + y_of[h] + BOX_XY * nby) & (BOX_XY - 1)).astype(F32) for h in range(2)]
    off_z = [((z0 + z_of[h] + BOX_Z * nbz) & (BOX_Z - 1)).astype(F32) for h in range(2)]

    def plane(j, carry):
        x = x0 + j - 2
        inside = jnp.where((x >= 0) & (x < nbx * BOX_XY), 1.0, 0.0)
        safe = jnp.clip(x, 0, nbx * BOX_XY - 1)
        bx = lax.div(safe, BOX_XY)
        off_x = lax.rem(safe, BOX_XY).astype(F32)

        def field(table, base, h, g):
            def one(by, bz):
                return table[base + (bx * nby + by) * nbz + bz].astype(F32)

            upper = jnp.where(
                low_lane,
                one(row_boxes[h][0], lane_boxes[g][0]),
                one(row_boxes[h][0], lane_boxes[g][1]),
            )
            if h == 0:
                return upper
            lower = jnp.where(
                low_lane,
                one(row_boxes[h][1], lane_boxes[g][0]),
                one(row_boxes[h][1], lane_boxes[g][1]),
            )
            return jnp.where(low_row, upper, lower)

        for h in range(2):
            for g in range(2):
                bits = jnp.zeros((8, 128), F32)
                for moment in range(3):
                    base = moment * 3 * boxes
                    gap_x = off_x - field(centers, base, h, g)
                    gap_y = off_y[h] - field(centers, base + boxes, h, g)
                    gap_z = off_z[g] - field(centers, base + 2 * boxes, h, g)
                    distance = gap_x * gap_x + gap_y * gap_y + gap_z * gap_z
                    hit = (distance <= float(RADIUS * RADIUS)) & (inside > 0.5)
                    bits = bits + jnp.where(hit, float(1 << moment), 0.0)
                code[j, h, g] = bits
                for d in range(3):
                    wind[d, j, h, g] = field(velocity, d * boxes, h, g) * inside
        return carry

    lax.fori_loop(0, 8, plane, 0)


def turned(tiles, step, axis):
    size = 8 if axis == 0 else 128
    at = iota2((8, 128), axis)
    rolled = [pltpu.roll(t, step % size, axis) for t in tiles]
    seam = at == (0 if step == 1 else size - 1)
    return [jnp.where(seam, rolled[1], rolled[0]), jnp.where(seam, rolled[0], rolled[1])]


def pull(tiles, cy, cz):
    if cz:
        tiles = [turned(tiles[h], cz, 1) for h in range(2)]
    if cy:
        first = turned([tiles[0][0], tiles[1][0]], cy, 0)
        second = turned([tiles[0][1], tiles[1][1]], cy, 0)
        tiles = [[first[0], second[0]], [first[1], second[1]]]
    return tiles


def main_kernel(ext_a, cext, z_l, z_r, code, wind, fine_next, coarse_next, force, ext_b, post, sums):
    gx, gz = lax.axis_index(GX), lax.axis_index("gz")
    last = lax.axis_size(GX) - 1
    row, lane = iota2((8, 128), 0), iota2((8, 128), 1)

    for k in range(5):
        q = ZP[k]
        for x in range(4):
            j = 1 + x - VELOCITIES[q][0]
            tile = jnp.where(lane == 127, pltpu.roll(z_l[j, 0:8], 31 - k, 1), cext[q, j])
            tile = pltpu.roll(tile, 1, 1)
            if VELOCITIES[q][1]:
                tile = pltpu.roll(tile, VELOCITIES[q][1] % 8, 0)
            coarse_next[q, x] = tile[0:4, 0:64]
        q = ZM[k]
        for x in range(4):
            j = 1 + x - VELOCITIES[q][0]
            tile = pltpu.roll(z_r[j, 0:8], 96 - k, 1)
            tile = jnp.where(lane == 64, tile, cext[q, j])
            tile = pltpu.roll(tile, 127, 1)
            if VELOCITIES[q][1]:
                tile = pltpu.roll(tile, VELOCITIES[q][1] % 8, 0)
            coarse_next[q, x] = tile[0:4, 0:64]
    for q in range(19):
        if VELOCITIES[q][2] == 0:
            for x in range(4):
                tile = cext[q, 1 + x - VELOCITIES[q][0]]
                if VELOCITIES[q][1]:
                    tile = pltpu.roll(tile, VELOCITIES[q][1] % 8, 0)
                coarse_next[q, x] = tile[0:4, 0:64]

    def unpack(j, carry):
        for h in range(2):
            from_l = z_l[j, 8 * h : 8 * h + 8]
            from_r = z_r[j, 8 * h : 8 * h + 8]
            both = jnp.where((lane & 2) == 0, from_l, from_r)
            for f in range(20):
                ext_b[f, j, 8 * h : 8 * h + 8] = pltpu.roll(both, (126 - 4 * f) % 128, 1)
        return carry

    lax.fori_loop(0, 8, unpack, 0)

    def substep(get, prev_bit, new_bit, first, stop, store, halves):
        def bits(j, h, g):
            return code[j, h, g].astype(jnp.int32)

        def prepare(j, carry):
            rho_open, open_ = [[None] * 2, [None] * 2], [[None] * 2, [None] * 2]
            for h in range(2):
                for g in range(2):
                    is_open = (bits(j, h, g) & (prev_bit | new_bit)) == 0
                    open_[h][g] = jnp.where(is_open, 1.0, 0.0)
                    rho_open[h][g] = jnp.where(is_open, get(RHO, j, h, g), 0.0)
            for n, tiles in enumerate((rho_open, open_)):
                back, forth = pull(tiles, 0, 1), pull(tiles, 0, -1)
                side_z = [[back[h][g] + forth[h][g] for g in range(2)] for h in range(2)]
                down, up = pull(tiles, 1, 0), pull(tiles, -1, 0)
                down2, up2 = pull(side_z, 1, 0), pull(side_z, -1, 0)
                for h in halves:
                    for g in halves:
                        side_y = down[h][g] + up[h][g]
                        both = down2[h][g] + up2[h][g]
                        sums[2 * n, j, h, g] = 2.0 * (side_y + side_z[h][g]) + both
                        sums[2 * n + 1, j, h, g] = 2.0 * tiles[h][g] + side_y + side_z[h][g]
            return carry

        lax.fori_loop(first - 1, stop + 1, prepare, 0)

        def plane(j, carry):
            pushes = list(carry)
            mine = [[bits(j, h, g) for g in range(2)] for h in range(2)]
            rho = [[get(RHO, j, h, g) for g in range(2)] for h in range(2)]
            covered, uncovered, refill = {}, {}, {}
            for h in halves:
                for g in halves:
                    covered[h, g] = (mine[h][g] & new_bit) != 0
                    uncovered[h, g] = (mine[h][g] & prev_bit) != 0
                    above = (
                        12.0 * rho[h][g]
                        + sums[0, j, h, g]
                        + (sums[1, j - 1, h, g] + sums[1, j + 1, h, g])
                    )
                    below = 12.0 + sums[2, j, h, g] + (sums[3, j - 1, h, g] + sums[3, j + 1, h, g])
                    density = above / below
                    own = [wind[d, j, h, g] for d in range(3)]
                    refill[h, g] = equilibria(density, own)
            own = [wind[d, j, 0, 0] for d in range(3)]
            for q in range(19):
                cx, cy, cz = VELOCITIES[q]
                weight = 6.0 * WEIGHTS[q]
                if q == 0:
                    for h in halves:
                        for g in halves:
                            p0 = get(0, j, h, g)
                            kept = jnp.where(uncovered[h, g], refill[h, g][0], p0)
                            store(0, j, h, g, jnp.where(covered[h, g], p0, kept))
                    continue
                src = j - cx
                ghost = jnp.logical_or(
                    jnp.logical_and(gx == 0, src < 2), jnp.logical_and(gx == last, src > 5)
                )
                fluid = jnp.where(ghost, 2.0 * BIG, BIG)
                state = [[None] * 2, [None] * 2]
                for h in range(2):
                    for g in range(2):
                        b = bits(src, h, g)
                        push = weight * along([wind[d, src, h, g] for d in range(3)], q)
                        state[h][g] = jnp.where(
                            (b & new_bit) != 0,
                            push,
                            jnp.where((b & prev_bit) != 0, 2.0 * BIG, fluid),
                        )
                state = pull(state, cy, cz)
                came = pull(
                    [[get(q, src, h, g) for g in range(2)] for h in range(2)], cy, cz
                )
                for h in halves:
                    for g in halves:
                        bounced = (
                            get(OPPOSITE[q], j, h, g) + state[h][g] * rho[h][g]
                        )
                        arrived = jnp.where(state[h][g] < 0.5 * BIG, bounced, came[h][g])
                        kept = jnp.where(uncovered[h, g], refill[h, g][q], arrived)
                        store(q, j, h, g, jnp.where(covered[h, g], get(q, j, h, g), kept))
                dens = pull([[get(RHO, src, h, g) for g in range(2)] for h in range(2)], cy, cz)
                term = 2.0 * came[0][0] - (weight * along(own, q)) * dens[0][0]
                linked = (state[0][0] > 0.5 * BIG) & (state[0][0] < 1.5 * BIG) & covered[0, 0]
                term = jnp.where(linked, term, 0.0)
                for d in range(3):
                    if VELOCITIES[q][d] == 1:
                        pushes[d] = pushes[d] + term
                    elif VELOCITIES[q][d] == -1:
                        pushes[d] = pushes[d] - term
            keep = jnp.logical_and(j >= 2, j <= 5)
            return tuple(jnp.where(keep, new, old) for new, old in zip(pushes, carry))

        zero = jnp.zeros((8, 128), F32)
        return lax.fori_loop(first, stop, plane, (zero, zero, zero))

    def get_first(f, j, h, g):
        return (ext_a, ext_b)[g][f, j, 8 * h : 8 * h + 8]

    def get_second(f, j, h, g):
        return post[f, j, h, g]

    def store_first(q, j, h, g, value):
        post[q, j, h, g] = value

    def store_second(q, j, h, g, value):
        fine_next[q, j - 2] = value

    first = substep(get_first, 1, 2, 1, 7, store_first, (0, 1))

    def relax(j, carry):
        for h in range(2):
            for g in range(2):
                out, density = collided([post[q, j, h, g] for q in range(19)], FINE_RATE)
                for q in range(19):
                    post[q, j, h, g] = out[q]
                post[RHO, j, h, g] = density
        return carry

    lax.fori_loop(1, 7, relax, 0)
    for edge, j in ((0, 1), (last, 6)):

        @pl.when(gx == edge)
        def _():
            for h in range(2):
                for g in range(2):
                    for f in range(20):
                        post[f, j, h, g] = get_first(f, j, h, g)

    second = substep(get_second, 2, 4, 2, 6, store_second, (0,))
    line = iota2((1, 128), 1)
    total = jnp.zeros((1, 128), F32)
    for n, value in enumerate(first + second):
        columns = jnp.sum(value, axis=0, keepdims=True)
        low = jnp.sum(jnp.where(line < 64, columns, 0.0), axis=1, keepdims=True)
        high = jnp.sum(jnp.where(line >= 64, columns, 0.0), axis=1, keepdims=True)
        at = n * 16 + 2 * gz
        total = jnp.where(line == at, low, jnp.where(line == at + 1, high, total))
    force[...] = jnp.broadcast_to(total, (32, 128))


def spread_kernel(got, out):
    out[...] = jnp.broadcast_to(jnp.sum(got[...], axis=0, keepdims=True), out.shape)


def boxes_kernel(got, out):
    b, r = iota2((16, 32), 0), iota2((16, 32), 1)
    pick = jnp.where(((b >> 2) == (r >> 3)) & ((b & 3) == (r & 3)), 1.0, 0.0)
    table = dot(pick, got[...])
    for n in range(6):
        rolled = pltpu.roll(table, (128 - 16 * n) % 128, 1) if n else table
        for bx in range(4):
            out[n // 3, n % 3, bx] = rolled[4 * bx : 4 * bx + 4, 0:16]


def call(kernel, shapes, operands, specs=None, scratch=(), name=None, keep=True, near=None):
    near = [s is not SMEM for s in specs or [VMEM] * len(operands)] if near is None else near
    operands = [
        pltpu.with_memory_space_constraint(x, pltpu.VMEM) if n else x
        for x, n in zip(operands, near)
    ]
    return pl.pallas_call(
        kernel,
        out_shape=[(pltpu.VMEM if keep else jax.ShapeDtypeStruct)(s, F32) for s in shapes],
        in_specs=specs or [VMEM] * len(operands),
        out_specs=[VMEM] * len(shapes),
        scratch_shapes=list(scratch),
        compiler_params=pltpu.CompilerParams(vmem_limit_bytes=24 * 2**20),
        name=name,
    )(*operands)


def swapped(up, down, axis):
    count = lax.axis_size(axis)
    from_low = lax.ppermute(up, axis, [(i, (i + 1) % count) for i in range(count)])
    from_high = lax.ppermute(down, axis, [((i + 1) % count, i) for i in range(count)])
    return from_low, from_high


def shards(coarse_pdfs, fine_pdfs, centers, sphere_velocity):
    fp, cp, xr, xl = call(
        collide_kernel,
        ((20, 4, 8, 128), (19, 4, 8, 128), (30, 8, 128), (30, 8, 128)),
        [pltpu.with_memory_space_constraint(x, pltpu.HBM) for x in (fine_pdfs, coarse_pdfs)],
        specs=[ANY, ANY],
        near=[False] * 2,
        scratch=(
            pltpu.VMEM(fine_pdfs.shape, F32),
            pltpu.VMEM(coarse_pdfs.shape, F32),
            pltpu.SemaphoreType.DMA((2,)),
        ),
        name="collide",
    )
    code, wind = call(
        geometry_kernel,
        ((8, 2, 2, 8, 128), (3, 8, 2, 2, 8, 128)),
        (centers.reshape(-1), sphere_velocity.reshape(-1), xr),
        specs=[SMEM, SMEM, ANY],
        name="geometry",
    )
    r_l, r_r = swapped(xr, xl, GX)
    yr, yl = call(
        pack_y_kernel,
        ((31, 8, 128), (31, 8, 128)),
        (fp, cp, r_l, r_r, code),
        specs=[VMEM] * 4 + [ANY],
        name="pack_y",
    )
    y_l, y_r = swapped(yr, yl, GY)
    ext, cext, zr, zl = call(
        pack_z_kernel,
        ((20, 8, 16, 128), (19, 6, 8, 128), (8, 16, 128), (8, 16, 128)),
        (fp, cp, r_l, r_r, y_l, y_r),
        name="pack_z",
    )
    z_l, z_r = swapped(zr, zl, "gz")
    fine_next, coarse_next, force = call(
        main_kernel,
        (fine_pdfs.shape, coarse_pdfs.shape, (32, 128)),
        (ext, cext, z_l, z_r, code, wind),
        keep=False,
        scratch=(
            pltpu.VMEM((20, 8, 16, 128), F32),
            pltpu.VMEM((20, 8, 2, 2, 8, 128), F32),
            pltpu.VMEM((4, 8, 2, 2, 8, 128), F32),
        ),
        name="main",
    )
    column = lax.all_to_all(force, ("gx_1", "gy_1", "gz"), 0, 0, tiled=True)
    (rows,) = call(spread_kernel, ((32, 128),), (column,), near=[False], name="spread", keep=False)
    rows = lax.all_to_all(rows, ("gx_0", "gy_0"), 0, 0, tiled=True)
    (sphere_force,) = call(boxes_kernel, ((2, 3, 4, 4, 16),), (rows,), near=[False], name="boxes", keep=False)
    return coarse_next, fine_next, sphere_force


def solution(mesh):
    split = Mesh(
        mesh.devices.reshape(8, 2, 4, 2, mesh.shape["gz"]), ("gx_0", "gx_1", "gy_0", "gy_1", "gz")
    )
    return jax.shard_map(
        shards,
        mesh=split,
        in_specs=(P(None, GX, GY, "gz"), P(None, GX, GY, "gz"), P(), P()),
        out_specs=(P(None, GX, GY, "gz"), P(None, GX, GY, "gz"), P()),
        check_vma=False,
    )
```
